512 devices in a mesh: cand: 16 (over y, z_hi, core), hid: 32 (over z_lo, x).
Axes of the slice: x: 4, y: 4, z: 16 (z_hi: 2, z_lo: 8; z = z_hi * 8 + z_lo), core: 2. Of those that a mesh axis runs over, the one named last changes fastest.
Arguments:
- tokens: bfloat16 [16, 256, 2048], P('cand', None, 'hid'), may hold values from -6 to 6
- cotangent: bfloat16 [16, 256, 2048], P('cand', None, 'hid'), may hold values from -6 to 6
- gate_weight: bfloat16 [2048, 8192], P('cand', 'hid'), may hold values from -0.125 to 0.125
- up_weight: bfloat16 [2048, 8192], P('cand', 'hid'), may hold values from -0.125 to 0.125
- down_weight: bfloat16 [8192, 2048], P('hid', 'cand'), may hold values from -0.125 to 0.125
- width_steps: int32 [16], P('cand'), may hold values from 1 to 8
- block_order: int32 [32], replicated, may hold values from 0 to 31, each once
Outputs:
- grad_tokens: float32 [16, 256, 2048], P('cand', None, 'hid')
- grad_gate: float32 [2048, 8192], P('cand', 'hid')
- grad_up: float32 [2048, 8192], P('cand', 'hid')
- grad_down: float32 [8192, 2048], P('hid', 'cand')
The draws below stay inside these ranges and needn't reach their ends.
Inputs may be any that keep to these rules, and one draw needn't show every extreme that they name: Candidate c uses the first width_steps[c] * 1024 logical hidden units. `block_order`: names each of the 32 logical blocks once.
All inputs are finite; a program needn't handle non-finite values.
Results may differ from the reference program's by a relative error of at most 0.02.
Values may be sent and summed in bfloat16 or wider, within the bound.
No kernel may reach another device: no remote copies, remote signals or barrier semaphores. Data moves between devices by JAX's collectives and lax.ppermute only.
A program may use at most 64 MiB of HBM per device.

```python
import jax
import jax.numpy as jnp
from jax import lax

D = 2048
FF = 8192
TOK = 256
CAND = 16
NBLK = 32
N_HID = 32


def place_ends(entries, key, smallest, high):
    place = [jax.random.randint(jax.random.fold_in(key, axis), (), 0, length) for axis, length in enumerate(entries.shape)]
    widest = entries.shape.index(max(entries.shape))
    neighbour = place[:widest] + [(place[widest] + 1) % entries.shape[widest]] + place[widest + 1:]
    return entries.at[tuple(place)].set(smallest).at[tuple(neighbour)].set(high)


def raised(drawn, stream_key, source, target, blocks, factor):
    owner, partner = [(jnp.arange(drawn.shape[position]) // (drawn.shape[position] // blocks)).reshape([-1 if axis == position else 1 for axis in range(drawn.ndim)]) for position in (source, target)]
    chosen = jax.random.permutation(stream_key, blocks)[partner]
    strong = (owner == chosen) | (owner == (partner + blocks // 2) % blocks)
    return jnp.where(strong, factor * drawn, drawn)


def steps_of(stream_key, shape, pieces, least, largest):
    def one(dim, blocks):
        heights = jax.random.uniform(jax.random.fold_in(jax.random.fold_in(stream_key, 6), dim), (blocks,), jnp.float32, least / len(pieces), largest / len(pieces))
        return jnp.repeat(jnp.exp(heights), shape[dim] // blocks).reshape((-1,) + (1,) * (len(shape) - dim - 1))

    loudness = one(*pieces[0])
    for cut in pieces[1:]:
        loudness = loudness * one(*cut)
    return loudness


def centred(key, dims, spread, most, shards=(), held_as=jnp.bfloat16):
    values = jax.random.normal(key, dims, jnp.float32) * spread
    if len(shards) > 0:
        values = steps_of(key, dims, shards, -0.22, 0.18) * values
    return jnp.clip(values, min=-most, max=most).astype(held_as)


def noise_with(key, dims, deviation, bound, shards, heavy, kind=jnp.bfloat16):
    entries = deviation * jax.random.normal(key, dims, jnp.float32)
    if shards:
        entries = entries * steps_of(key, dims, shards, -0.22, 0.18)
    return jnp.clip(raised(entries, jax.random.fold_in(key, 3), *heavy), -bound, bound).astype(kind)


def setup_inputs(seed: int = 0) -> dict:
    arg_keys = jax.random.split(jax.random.key(seed), 8)
    tokens = centred(arg_keys[0], (CAND, TOK, D), 1.0, 6.0, ((0, 16), (2, 32)))
    cotangent = noise_with(arg_keys[1], (CAND, TOK, D), 1.0, 6.0, ((0, 16), (2, 32)), (0, 2, 16, 2.0))
    gate_weight = centred(arg_keys[2], (D, FF), D ** -0.5, 0.125, ((0, 16), (1, 32)))
    up_weight = centred(arg_keys[3], (D, FF), D ** -0.5, 0.125, ((0, 16), (1, 32)))
    down_weight = centred(arg_keys[4], (FF, D), (FF // 4) ** -0.5, 0.125, ((0, 32), (1, 16)))
    width_steps = place_ends(jax.random.randint(arg_keys[5], (CAND,), 1, 9), jax.random.fold_in(arg_keys[5], 1), 1, 8).astype(jnp.int32)
    block_order = jax.random.permutation(arg_keys[6], NBLK).astype(jnp.int32)
    return {"tokens": tokens, "cotangent": cotangent, "gate_weight": gate_weight, "up_weight": up_weight, "down_weight": down_weight, "width_steps": width_steps, "block_order": block_order}


def reference(tokens, cotangent, gate_weight, up_weight, down_weight, width_steps, block_order):
    blk = FF // N_HID
    column = jnp.arange(FF, dtype=jnp.int32)
    logical = block_order[column // blk].astype(jnp.int32) * blk + column % blk
    gate_wide = gate_weight.astype(jnp.float32).reshape(D, N_HID, blk)
    up_wide = up_weight.astype(jnp.float32).reshape(D, N_HID, blk)

    def one(carry, index):
        inputs = tokens[index]
        upstream = cotangent[index]
        keep = (logical < width_steps[index] * (FF // 8)).astype(jnp.float32)
        gate = jnp.dot(inputs, gate_weight, preferred_element_type=jnp.float32)
        up = jnp.dot(inputs, up_weight, preferred_element_type=jnp.float32)
        sig = jax.nn.sigmoid(gate)
        act = keep * gate * sig
        hidden = (act * up).astype(jnp.bfloat16)
        dhid = keep * jnp.dot(upstream, down_weight.T, preferred_element_type=jnp.float32)
        d_up = (dhid * act).astype(jnp.bfloat16)
        d_gate = (dhid * up * keep * sig * (1.0 + gate * (1.0 - sig))).astype(jnp.bfloat16)
        down_c = jnp.dot(hidden.T, upstream, preferred_element_type=jnp.float32).astype(jnp.bfloat16).astype(jnp.float32)
        gate_c = jnp.dot(inputs.T, d_gate, preferred_element_type=jnp.float32).astype(jnp.bfloat16).astype(jnp.float32)
        up_c = jnp.dot(inputs.T, d_up, preferred_element_type=jnp.float32).astype(jnp.bfloat16).astype(jnp.float32)
        dg3 = d_gate.astype(jnp.float32).reshape(TOK, N_HID, blk)
        du3 = d_up.astype(jnp.float32).reshape(TOK, N_HID, blk)
        parts = jnp.einsum('tkb,dkb->ktd', dg3, gate_wide) + jnp.einsum('tkb,dkb->ktd', du3, up_wide)
        grad_in = jnp.sum(parts.astype(jnp.bfloat16).astype(jnp.float32), axis=0)
        return (carry[0] + gate_c, carry[1] + up_c, carry[2] + down_c), grad_in

    start = (jnp.zeros((D, FF), jnp.float32), jnp.zeros((D, FF), jnp.float32), jnp.zeros((FF, D), jnp.float32))
    sums, grad_tokens = lax.scan(one, start, jnp.arange(CAND, dtype=jnp.int32))
    return grad_tokens, sums[0], sums[1], sums[2]
```

```python
import jax
import jax.numpy as jnp
from jax import lax
from jax.experimental import pallas as pl
from jax.experimental.pallas import tpu as pltpu
from jax.sharding import PartitionSpec as P

FF = 8192
TOK = 256
LANES = 128
BLK = 256
Z_OFFSETS = (0, 4, 2, 6, 1, 5, 3, 7)


VMEM = pl.BlockSpec(memory_space=pltpu.VMEM)
SMEM = pl.BlockSpec(memory_space=pltpu.SMEM)
F32 = jnp.float32
BF16 = jnp.bfloat16


def swap(v, axis, size, offset):
    return lax.ppermute(v, axis, [(k, k ^ offset) for k in range(size)])


def halves_mask(shape, parity):
    lane = lax.broadcasted_iota(jnp.int32, shape, len(shape) - 1)
    return (lane < LANES // 2) == (parity == 0)


def forward_kernel(place, keep_ref, x0, x1, x2, x3, a0, a1, a2, a3, b0, b1, b2, b3,
                   tok, cot, dgu, hid, g0, g1, g2, g3):
    z, x_hi, parity, c0 = place[0], place[1], place[2], place[3]
    mask = halves_mask((TOK, LANES), parity)
    for half, (even, odd) in enumerate(((x0, x1), (x2, x3))):
        for s, a in enumerate(Z_OFFSETS):
            block = ((z ^ a) * 2 + (x_hi ^ half)) ^ c0
            at = (block & 1) * 8 + lax.shift_right_logical(block, 1)
            lanes = pl.ds(pl.multiple_of(at * LANES, LANES), LANES)
            e, o = even[s], odd[s]
            tok[:, lanes] = jnp.where(mask, e, o)
            cot[:, lanes] = jnp.where(mask, o, e)
    weights = (a0, a1, a2, a3, b0, b1, b2, b3)
    gate_up = jnp.zeros((TOK, 2 * BLK), F32)
    dhid = jnp.zeros((TOK, BLK), F32)
    for k, w in enumerate(weights):
        cols = slice(k * 256, (k + 1) * 256)
        wk = w[...].reshape(256, 3 * BLK)
        gate_up += jnp.dot(tok[:, cols], wk[:, : 2 * BLK], preferred_element_type=F32)
        dhid += jnp.dot(cot[:, cols], wk[:, 2 * BLK :], preferred_element_type=F32)
    keep = keep_ref[0]
    gate, up = gate_up[:, :BLK], gate_up[:, BLK:]
    sig = jax.nn.sigmoid(gate)
    act = keep * gate * sig
    dhid = keep * dhid
    hid[...] = (act * up).astype(BF16)
    dgu[:, BLK:] = (dhid * act).astype(BF16)
    dgu[:, :BLK] = (dhid * up * keep * sig * (1.0 + gate * (1.0 - sig))).astype(BF16)
    weight_grads(tok, cot, dgu, hid, (g0, g1, g2, g3), 1024)


def weight_grads(tok, cot, dgu, hid, outs, first):
    dims = (((0,), (0,)), ((), ()))
    for k, out in enumerate(outs):
        cols = slice(first + k * 256, first + (k + 1) * 256)
        gu = lax.dot_general(tok[:, cols], dgu[...], dims, preferred_element_type=F32)
        dn = lax.dot_general(cot[:, cols], hid[...], dims, preferred_element_type=F32)
        out[:, :, : 2 * BLK] = gu.astype(BF16).reshape(2, 128, 2 * BLK)
        out[:, :, 2 * BLK :] = dn.astype(BF16).reshape(2, 128, BLK)


def own_grads_kernel(tok, cot, dgu, hid, g0, g1, g2, g3):
    weight_grads(tok, cot, dgu, hid, (g0, g1, g2, g3), 0)


def token_grads_kernel(place, dgu, a0, a1, a2, a3, b0, b1, b2, b3, r0, r1, r2, r3, parts):
    z, x_hi, parity, c0 = place[0], place[1], place[2], place[3]
    dims = (((1,), (1,)), ((), ()))
    for k, w in enumerate((a0, a1, a2, a3, b0, b1, b2, b3)):
        wk = w[...].reshape(256, 3 * BLK)[:, : 2 * BLK]
        part = lax.dot_general(dgu[...], wk, dims, preferred_element_type=F32)
        for j in range(2):
            at = 2 * k + j
            parts[c0 ^ ((at % 8) * 2 + at // 8)] = part[:, j * LANES : (j + 1) * LANES]
    mask = halves_mask((TOK // 2, LANES), parity)
    for half, (same, other) in enumerate(((r0, r1), (r2, r3))):
        for s, a in enumerate(Z_OFFSETS):
            part = parts[(z ^ a) * 2 + (x_hi ^ half)]
            top = part[: TOK // 2]
            low = pltpu.roll(part[TOK // 2 :], LANES // 2, 1)
            same[s] = jnp.where(mask, top, low).astype(BF16)
            other[s] = jnp.where(mask, low, top).astype(BF16)


def call(kernel, outs, n_smem, n_in, scratch=()):
    return pl.pallas_call(
        kernel,
        out_shape=outs,
        in_specs=[SMEM] * n_smem + [VMEM] * n_in,
        out_specs=[VMEM] * len(outs),
        scratch_shapes=list(scratch),
        compiler_params=pltpu.CompilerParams(vmem_limit_bytes=48 * 1024 * 1024),
    )


def sds(*shape, dtype=BF16):
    return jax.ShapeDtypeStruct(shape, dtype)


def shards(tokens, cotangent, gate_weight, up_weight, down_weight, width_steps, block_order):
    c, h = lax.axis_index("cand"), lax.axis_index("hid")
    z, x = h // 4, h % 4
    parity = x % 2
    place = jnp.stack([z, x // 2, parity, c]).astype(jnp.int32)
    places = jnp.arange(block_order.shape[0], dtype=jnp.int32)
    logical = jnp.sum(jnp.where(places == h, block_order, 0))
    keep = (logical * BLK < width_steps[0] * (FF // 8)).astype(F32).reshape(1)

    t, u = tokens[0], cotangent[0]
    first, second = jnp.where(parity == 0, t, u), jnp.where(parity == 0, u, t)
    piece = jnp.concatenate([first, second], axis=1)[None]
    down_t = down_weight.T
    down_t = jnp.concatenate([down_t[64:], down_t[:64]], axis=0)
    shard = jnp.concatenate([gate_weight, up_weight, down_t], axis=1)

    far = swap(shard, "cand", 16, 2)
    for step in (4, 2, 1):
        piece = jnp.concatenate([piece, swap(piece, "hid", 32, 4 * step)], axis=0)
    pair = jnp.stack([shard, far])
    xs = [piece] + [swap(piece, "hid", 32, b) for b in (1, 2, 3)]
    mine = [pair] + [swap(pair, "cand", 16, 4 * i) for i in (1, 2, 3)]
    theirs = [swap(w, "cand", 16, 1) for w in mine]

    grad = sds(2, 128, 3 * BLK)
    tok, cot, dgu, hid, *away = call(
        forward_kernel,
        [sds(TOK, 2048), sds(TOK, 2048), sds(TOK, 2 * BLK), sds(TOK, BLK)] + [grad] * 4, 2, 12,
    )(place, keep, *xs, *mine, *theirs)
    arrived = [swap(g, "cand", 16, 1) for g in away]
    own = call(own_grads_kernel, [grad] * 4, 0, 4)(tok, cot, dgu, hid)
    r0, *rs = call(
        token_grads_kernel, [sds(8, 128, 128)] * 4, 1, 9, [pltpu.VMEM((16, TOK, LANES), F32)]
    )(place, dgu, *mine, *theirs)

    both = [a.astype(F32) + b.astype(F32) for a, b in zip(own, arrived)]
    total = both[0]
    for i in (1, 2, 3):
        total = total + swap(both[i].astype(BF16), "cand", 16, 4 * i).astype(F32)
    grads = total[0] + swap(total[1].astype(BF16), "cand", 16, 2).astype(F32)

    part = r0.astype(F32)
    for b, r in zip((1, 2, 3), rs):
        part = part + swap(r, "hid", 32, b).astype(F32)
    for step in (1, 2, 4):
        n = part.shape[0] // 2
        part = part[:n] + swap(part[n:].astype(BF16), "hid", 32, 4 * step).astype(F32)
    left, right = part[0, :, :64], part[0, :, 64:]
    top, low = jnp.where(parity == 0, left, right), jnp.where(parity == 0, right, left)
    grad_tokens = jnp.concatenate([top, low], axis=0)[None]

    grad_down = grads[:, 2 * BLK :]
    grad_down = jnp.concatenate([grad_down[64:], grad_down[:64]], axis=0).T
    return grad_tokens, grads[:, :BLK], grads[:, BLK : 2 * BLK], grad_down


def solution(mesh):
    in_specs = (
        P("cand", None, "hid"),
        P("cand", None, "hid"),
        P("cand", "hid"),
        P("cand", "hid"),
        P("hid", "cand"),
        P("cand"),
        P(),
    )
    out_specs = (P("cand", None, "hid"), P("cand", "hid"), P("cand", "hid"), P("hid", "cand"))
    return jax.shard_map(shards, mesh=mesh, in_specs=in_specs, out_specs=out_specs, check_vma=False)
```

```python
import jax
import jax.numpy as jnp
from jax import lax
from jax.experimental import pallas as pl
from jax.experimental.pallas import tpu as pltpu
from jax.sharding import PartitionSpec as P

FF = 8192
TOK = 256
LANES = 128
BLK = 256
Y_GROUPS = [[4 * y + r for y in range(4)] for r in range(4)]
Z_GROUPS = [[8 * q + r for q in range(4)] for r in range(8)]


VMEM = pl.BlockSpec(memory_space=pltpu.VMEM)
SMEM = pl.BlockSpec(memory_space=pltpu.SMEM)
F32 = jnp.float32
BF16 = jnp.bfloat16


def swap(v, axis, offset):
    return lax.ppermute(v, axis, [(k, k ^ offset) for k in range(lax.axis_size(axis))])


def exchange(v, axis, groups):
    return lax.all_to_all(v, axis, 0, 0, axis_index_groups=groups, tiled=True)


def gather(v, axis, groups):
    return exchange(jnp.broadcast_to(v[None], (4, *v.shape)), axis, groups)


def total(v):
    return jnp.sum(v.astype(F32), axis=0)


def halves_mask(shape, parity):
    return (lax.broadcasted_iota(jnp.int32, shape, 1) < LANES // 2) == (parity == 0)


def forward_kernel(place, keep_ref, lo0, lo1, lo2, lo3, hi0, hi1, hi2, hi3, w0, w1, w2, w3,
                   own0, own1, away0, away1, dgu, tok, cot, hid):
    side, core, parity, quarter = place[0], place[1], place[2], place[3]
    mask = halves_mask((TOK, LANES), parity)
    pairs = ((lo0, lo1, 0, 0), (lo2, lo3, 1, 0), (hi0, hi1, 0, 1), (hi2, hi3, 1, 1))
    for even, odd, half, turn in pairs:
        chunk = (half ^ core) * 2 + (turn ^ side)
        for s, q in enumerate((0, 2, 1, 3)):
            lanes = pl.ds(pl.multiple_of((chunk * 4 + (quarter ^ q)) * LANES, LANES), LANES)
            e, f = even[s], odd[s]
            tok[:, lanes] = jnp.where(mask, e, f)
            cot[:, lanes] = jnp.where(mask, f, e)
    gate_up = jnp.zeros((TOK, 2 * BLK), F32)
    dhid = jnp.zeros((TOK, BLK), F32)
    for k, w in enumerate((w0, w1, w2, w3)):
        cols = slice(k * 512, (k + 1) * 512)
        wk = w[...].reshape(512, 3 * BLK)
        gate_up += jnp.dot(tok[:, cols], wk[:, : 2 * BLK], preferred_element_type=F32)
        dhid += jnp.dot(cot[:, cols], wk[:, 2 * BLK :], preferred_element_type=F32)
    keep = keep_ref[0]
    gate, up = gate_up[:, :BLK], gate_up[:, BLK:]
    sig = jax.nn.sigmoid(gate)
    act = keep * gate * sig
    dhid = keep * dhid
    hid[...] = (act * up).astype(BF16)
    dgu[:, BLK:] = (dhid * act).astype(BF16)
    dgu[:, :BLK] = (dhid * up * keep * sig * (1.0 + gate * (1.0 - sig))).astype(BF16)
    dims = (((0,), (0,)), ((), ()))
    for k, out in ((3, away1), (2, away0), (1, own1), (0, own0)):
        cols = slice(k * 512, (k + 1) * 512)
        gu = lax.dot_general(tok[:, cols], dgu[...], dims, preferred_element_type=F32)
        dn = lax.dot_general(cot[:, cols], hid[...], dims, preferred_element_type=F32)
        out[:, :, : 2 * BLK] = gu.astype(BF16).reshape(4, 128, 2 * BLK)
        out[:, :, 2 * BLK :] = dn.astype(BF16).reshape(4, 128, BLK)


def shard_kernel(gate, up, down, out):
    out[:, :BLK] = gate[...]
    out[:, BLK : 2 * BLK] = up[...]
    turned = down[...].T
    out[:64, 2 * BLK :] = turned[64:]
    out[64:, 2 * BLK :] = turned[:64]


def token_grads_kernel(place, dgu, w0, w1, w2, w3, out):
    side, core, parity = place[0], place[1], place[2]
    mask = halves_mask((TOK // 2, LANES), parity)
    dims = (((1,), (1,)), ((), ()))
    for k, w in enumerate((w0, w1, w2, w3)):
        wk = w[...].reshape(512, 3 * BLK)[:, : 2 * BLK]
        part = lax.dot_general(dgu[...], wk, dims, preferred_element_type=F32)
        x, turn = 2 * (k // 2 ^ core), k % 2 ^ side
        for q in range(4):
            block = part[:, q * LANES : (q + 1) * LANES]
            top = block[: TOK // 2]
            low = pltpu.roll(block[TOK // 2 :], LANES // 2, 1)
            out[x, turn, q] = jnp.where(mask, top, low).astype(BF16)
            out[x + 1, turn, q] = jnp.where(mask, low, top).astype(BF16)


def call(kernel, outs, n_smem, n_in, scratch, mib):
    run = pl.pallas_call(
        kernel,
        out_shape=outs,
        in_specs=[SMEM] * n_smem + [VMEM] * n_in,
        out_specs=[VMEM] * len(outs),
        scratch_shapes=list(scratch),
        compiler_params=pltpu.CompilerParams(vmem_limit_bytes=mib * 1024 * 1024),
    )
    return run


def sds(*shape, dtype=BF16):
    return jax.ShapeDtypeStruct(shape, dtype)


def step(tokens, cotangent, gate_weight, up_weight, down_weight, width_steps, block_order):
    c, h = lax.axis_index("cand"), lax.axis_index("hid")
    parity = h % 2
    place = jnp.stack([(h // 4 ^ c // 2) % 2, (c ^ h // 2) % 2, parity, h // 8]).astype(jnp.int32)
    places = jnp.arange(block_order.shape[0], dtype=jnp.int32)
    logical = jnp.sum(jnp.where(places == h, block_order, 0))
    keep = (logical * BLK < width_steps[0] * (FF // 8)).astype(F32).reshape(1)

    t, u = tokens[0], cotangent[0]
    first, second = jnp.where(parity == 0, t, u), jnp.where(parity == 0, u, t)
    piece = jnp.concatenate([first, second], axis=1)[None]
    (shard,) = call(shard_kernel, [sds(128, 3 * BLK)], 0, 3, [], 4)(
        gate_weight, up_weight, down_weight
    )

    pieces = jnp.concatenate([piece, swap(piece, "hid", 16)], axis=0)
    far = swap(shard, "cand", 2)
    w_own = gather(shard, "cand", Y_GROUPS)
    pieces = jnp.concatenate([pieces, swap(pieces, "hid", 8)], axis=0)
    pieces, place, keep = lax.optimization_barrier((pieces, place, keep))
    others = swap(pieces, "hid", 4)
    los = [pieces] + [swap(pieces, "hid", b) for b in (1, 2, 3)]
    his = [others] + [swap(others, "hid", b) for b in (1, 2, 3)]
    w_far = gather(far, "cand", Y_GROUPS)
    weights = [w_own, w_far, swap(w_own, "cand", 1), swap(w_far, "cand", 1)]

    grad = sds(4, 128, 3 * BLK)
    own0, own1, away0, away1, dgu = call(
        forward_kernel, [grad] * 4 + [sds(TOK, 2 * BLK)], 2, 12,
        [pltpu.VMEM((TOK, 2048), BF16)] * 2 + [pltpu.VMEM((TOK, BLK), BF16)], 12,
    )(place, keep, *los, *his, *weights)
    (parts,) = call(token_grads_kernel, [sds(4, 2, 4, 128, 128)], 1, 5, [], 8)(place, dgu, *weights)

    both1 = own1.astype(F32) + swap(away1, "cand", 1).astype(F32)
    total1 = total(exchange(both1.astype(BF16), "cand", Y_GROUPS))
    arrived0 = swap(away0, "cand", 1)
    both0 = (own0.astype(F32) + arrived0.astype(F32)).astype(BF16)
    grads = total(exchange(both0, "cand", Y_GROUPS))
    grads = grads + swap(total1.astype(BF16), "cand", 2).astype(F32)

    arrived = [swap(parts[b], "hid", b) for b in (1, 2, 3)]
    part = parts[0].astype(F32)
    for r in arrived:
        part = part + r.astype(F32)
    part = part[0] + swap(part[1].astype(BF16), "hid", 4).astype(F32)
    part = total(exchange(part.astype(BF16), "hid", Z_GROUPS))
    left, right = part[:, :64], part[:, 64:]
    top, low = jnp.where(parity == 0, left, right), jnp.where(parity == 0, right, left)
    grad_tokens = jnp.concatenate([top, low], axis=0)[None]

    grad_down = grads[:, 2 * BLK :]
    grad_down = jnp.concatenate([grad_down[64:], grad_down[:64]], axis=0).T
    return grad_tokens, grads[:, :BLK], grads[:, BLK : 2 * BLK], grad_down


def solution(mesh):
    in_specs = (
        P("cand", None, "hid"),
        P("cand", None, "hid"),
        P("cand", "hid"),
        P("cand", "hid"),
        P("hid", "cand"),
        P("cand"),
        P(),
    )
    out_specs = (P("cand", None, "hid"), P("cand", "hid"), P("cand", "hid"), P("hid", "cand"))
    return jax.shard_map(step, mesh=mesh, in_specs=in_specs, out_specs=out_specs, check_vma=False)
```

```python
import jax
import jax.numpy as jnp
from jax import lax
from jax.experimental import pallas as pl
from jax.experimental.pallas import tpu as pltpu
from jax.sharding import PartitionSpec as P

FF = 8192
TOK = 256
LANES = 128
BLK = 256
Y_GROUPS = [[4 * y + r for y in range(4)] for r in range(4)]
Z_OFFSETS = (0, 4, 2, 6, 1, 5, 3, 7)


VMEM = pl.BlockSpec(memory_space=pltpu.VMEM)
SMEM = pl.BlockSpec(memory_space=pltpu.SMEM)
F32 = jnp.float32
BF16 = jnp.bfloat16


def swap(v, axis, offset):
    return lax.ppermute(v, axis, [(k, k ^ offset) for k in range(lax.axis_size(axis))])


def exchange(v, axis, groups):
    return lax.all_to_all(v, axis, 0, 0, axis_index_groups=groups, tiled=True)


def gather(v, axis, groups):
    return exchange(jnp.broadcast_to(v[None], (4, *v.shape)), axis, groups)


def total(v):
    return jnp.sum(v.astype(F32), axis=0)


def halves_mask(shape, parity):
    return (lax.broadcasted_iota(jnp.int32, shape, 1) < LANES // 2) == (parity == 0)


def forward_kernel(place, keep_ref, x0, x1, x2, x3, w0, w1, w2, w3,
                   own0, own1, away0, away1, dgu, tok, cot, hid):
    side, core, parity, quarter = place[0], place[1], place[2], place[3]
    mask = halves_mask((TOK, LANES), parity)
    for half, (even, odd) in enumerate(((x0, x1), (x2, x3))):
        for s, a in enumerate(Z_OFFSETS):
            chunk = (half ^ core) * 2 + (a % 2 ^ side)
            lanes = pl.ds(pl.multiple_of((chunk * 4 + (quarter ^ a // 2)) * LANES, LANES), LANES)
            e, f = even[s], odd[s]
            tok[:, lanes] = jnp.where(mask, e, f)
            cot[:, lanes] = jnp.where(mask, f, e)
    gate_up = jnp.zeros((TOK, 2 * BLK), F32)
    dhid = jnp.zeros((TOK, BLK), F32)
    for k, w in enumerate((w0, w1, w2, w3)):
        cols = slice(k * 512, (k + 1) * 512)
        wk = w[...].reshape(512, 3 * BLK)
        gate_up += jnp.dot(tok[:, cols], wk[:, : 2 * BLK], preferred_element_type=F32)
        dhid += jnp.dot(cot[:, cols], wk[:, 2 * BLK :], preferred_element_type=F32)
    keep = keep_ref[0]
    gate, up = gate_up[:, :BLK], gate_up[:, BLK:]
    sig = jax.nn.sigmoid(gate)
    act = keep * gate * sig
    dhid = keep * dhid
    hid[...] = (act * up).astype(BF16)
    dgu[:, BLK:] = (dhid * act).astype(BF16)
    dgu[:, :BLK] = (dhid * up * keep * sig * (1.0 + gate * (1.0 - sig))).astype(BF16)
    dims = (((0,), (0,)), ((), ()))
    for k, out in ((3, away1), (2, away0), (1, own1), (0, own0)):
        cols = slice(k * 512, (k + 1) * 512)
        gu = lax.dot_general(tok[:, cols], dgu[...], dims, preferred_element_type=F32)
        dn = lax.dot_general(cot[:, cols], hid[...], dims, preferred_element_type=F32)
        out[:, :, : 2 * BLK] = gu.astype(BF16).reshape(4, 128, 2 * BLK)
        out[:, :, 2 * BLK :] = dn.astype(BF16).reshape(4, 128, BLK)


def shard_kernel(gate, up, down, out):
    out[:, :BLK] = gate[...]
    out[:, BLK : 2 * BLK] = up[...]
    turned = down[...].T
    out[:64, 2 * BLK :] = turned[64:]
    out[64:, 2 * BLK :] = turned[:64]


def token_grads_kernel(place, dgu, w0, w1, w2, w3, r0, r1, r2, r3):
    side, core, parity, quarter = place[0], place[1], place[2], place[3]
    mask = halves_mask((TOK // 2, LANES), parity)
    dims = (((1,), (1,)), ((), ()))

    def half(weights, same, other):
        for k, w in enumerate(weights):
            wk = w[...].reshape(512, 3 * BLK)[:, : 2 * BLK]
            part = lax.dot_general(dgu[...], wk, dims, preferred_element_type=F32)
            for y in range(4):
                q = quarter ^ y
                at = (k ^ side) * 4 + (q & 1) * 2 + lax.shift_right_logical(q, 1)
                block = part[:, y * LANES : (y + 1) * LANES]
                top = block[: TOK // 2]
                low = pltpu.roll(block[TOK // 2 :], LANES // 2, 1)
                same[at] = jnp.where(mask, top, low).astype(BF16)
                other[at] = jnp.where(mask, low, top).astype(BF16)

    for turn, (first, second) in enumerate((((w0, w1), (w2, w3)), ((w2, w3), (w0, w1)))):

        @pl.when(core == turn)
        def _(first=first, second=second):
            half(first, r0, r1)
            half(second, r2, r3)


def call(kernel, outs, n_smem, n_in, scratch, mib):
    run = pl.pallas_call(
        kernel,
        out_shape=outs,
        in_specs=[SMEM] * n_smem + [VMEM] * n_in,
        out_specs=[VMEM] * len(outs),
        scratch_shapes=list(scratch),
        compiler_params=pltpu.CompilerParams(vmem_limit_bytes=mib * 1024 * 1024),
    )
    return run


def sds(*shape, dtype=BF16):
    return jax.ShapeDtypeStruct(shape, dtype)


def step(tokens, cotangent, gate_weight, up_weight, down_weight, width_steps, block_order):
    c, h = lax.axis_index("cand"), lax.axis_index("hid")
    parity = h % 2
    place = jnp.stack([(h // 4 ^ c // 2) % 2, (c ^ h // 2) % 2, parity, h // 8]).astype(jnp.int32)
    places = jnp.arange(block_order.shape[0], dtype=jnp.int32)
    logical = jnp.sum(jnp.where(places == h, block_order, 0))
    keep = (logical * BLK < width_steps[0] * (FF // 8)).astype(F32).reshape(1)

    t, u = tokens[0], cotangent[0]
    first, second = jnp.where(parity == 0, t, u), jnp.where(parity == 0, u, t)
    piece = jnp.concatenate([first, second], axis=1)[None]
    (shard,) = call(shard_kernel, [sds(128, 3 * BLK)], 0, 3, [], 4)(
        gate_weight, up_weight, down_weight
    )

    pieces = jnp.concatenate([piece, swap(piece, "hid", 16)], axis=0)
    far = swap(shard, "cand", 2)
    w_own = gather(shard, "cand", Y_GROUPS)
    pieces = jnp.concatenate([pieces, swap(pieces, "hid", 8)], axis=0)
    pieces, place, keep = lax.optimization_barrier((pieces, place, keep))
    pieces = jnp.concatenate([pieces, swap(pieces, "hid", 4)], axis=0)
    xs = [pieces] + [swap(pieces, "hid", b) for b in (1, 2, 3)]
    w_far = gather(far, "cand", Y_GROUPS)
    weights = [w_own, w_far, swap(w_own, "cand", 1), swap(w_far, "cand", 1)]

    grad = sds(4, 128, 3 * BLK)
    own0, own1, away0, away1, dgu = call(
        forward_kernel, [grad] * 4 + [sds(TOK, 2 * BLK)], 2, 8,
        [pltpu.VMEM((TOK, 2048), BF16)] * 2 + [pltpu.VMEM((TOK, BLK), BF16)], 12,
    )(place, keep, *xs, *weights)
    r0, *rs = call(token_grads_kernel, [sds(8, 128, 128)] * 4, 1, 5, [], 8)(place, dgu, *weights)

    both1 = own1.astype(F32) + swap(away1, "cand", 1).astype(F32)
    total1 = total(exchange(both1.astype(BF16), "cand", Y_GROUPS))
    arrived0 = swap(away0, "cand", 1)
    both0 = (own0.astype(F32) + arrived0.astype(F32)).astype(BF16)
    grads = total(exchange(both0, "cand", Y_GROUPS))
    last = swap(total1.astype(BF16), "cand", 2)
    grads = lax.optimization_barrier(grads) + last.astype(F32)

    part = r0.astype(F32)
    for b, r in zip((1, 2, 3), rs):
        part = part + swap(r, "hid", b).astype(F32)
    for dist in (1, 2, 4):
        n = part.shape[0] // 2
        part = part[:n] + swap(part[n:].astype(BF16), "hid", 4 * dist).astype(F32)
    part = part[0]
    left, right = part[:, :64], part[:, 64:]
    top, low = jnp.where(parity == 0, left, right), jnp.where(parity == 0, right, left)
    grad_tokens = jnp.concatenate([top, low], axis=0)[None]

    grad_down = grads[:, 2 * BLK :]
    grad_down = jnp.concatenate([grad_down[64:], grad_down[:64]], axis=0).T
    return grad_tokens, grads[:, :BLK], grads[:, BLK : 2 * BLK], grad_down


def solution(mesh):
    in_specs = (
        P("cand", None, "hid"),
        P("cand", None, "hid"),
        P("cand", "hid"),
        P("cand", "hid"),
        P("hid", "cand"),
        P("cand"),
        P(),
    )
    out_specs = (P("cand", None, "hid"), P("cand", "hid"), P("cand", "hid"), P("hid", "cand"))
    return jax.shard_map(step, mesh=mesh, in_specs=in_specs, out_specs=out_specs, check_vma=False)
```

```python
import jax
import jax.numpy as jnp
from jax import lax
from jax.experimental import pallas as pl
from jax.experimental.pallas import tpu as pltpu
from jax.sharding import PartitionSpec as P

FF = 8192
TOK = 256
LANES = 128
BLK = 256
Y_GROUPS = [[4 * y + r for y in range(4)] for r in range(4)]
Z_OFFSETS = (0, 4, 2, 6)


VMEM = pl.BlockSpec(memory_space=pltpu.VMEM)
SMEM = pl.BlockSpec(memory_space=pltpu.SMEM)
F32 = jnp.float32
BF16 = jnp.bfloat16


def swap(v, axis, offset):
    return lax.ppermute(v, axis, [(k, k ^ offset) for k in range(lax.axis_size(axis))])


def exchange(v, axis, groups):
    return lax.all_to_all(v, axis, 0, 0, axis_index_groups=groups, tiled=True)


def gather(v, axis, groups):
    return exchange(jnp.broadcast_to(v[None], (4, *v.shape)), axis, groups)


def total(v):
    return jnp.sum(v.astype(F32), axis=0)


def halves_mask(shape, parity):
    return (lax.broadcasted_iota(jnp.int32, shape, 1) < LANES // 2) == (parity == 0)


def forward_kernel(place, keep_ref, lo0, lo1, lo2, lo3, hi0, hi1, hi2, hi3, w0, w1, w2, w3,
                   own0, own1, away0, away1, dgu, tok, cot, hid):
    side, core, parity, quarter = place[0], place[1], place[2], place[3]
    mask = halves_mask((TOK, LANES), parity)
    pairs = ((lo0, lo1, 0, 0), (lo2, lo3, 1, 0), (hi0, hi1, 0, 1), (hi2, hi3, 1, 1))
    for even, odd, half, turn in pairs:
        chunk = (half ^ core) * 2 + (turn ^ side)
        for s, a in enumerate(Z_OFFSETS):
            lanes = pl.ds(pl.multiple_of((chunk * 4 + (quarter ^ a // 2)) * LANES, LANES), LANES)
            e, f = even[s], odd[s]
            tok[:, lanes] = jnp.where(mask, e, f)
            cot[:, lanes] = jnp.where(mask, f, e)
    gate_up = jnp.zeros((TOK, 2 * BLK), F32)
    dhid = jnp.zeros((TOK, BLK), F32)
    for k, w in enumerate((w0, w1, w2, w3)):
        cols = slice(k * 512, (k + 1) * 512)
        wk = w[...].reshape(512, 3 * BLK)
        gate_up += jnp.dot(tok[:, cols], wk[:, : 2 * BLK], preferred_element_type=F32)
        dhid += jnp.dot(cot[:, cols], wk[:, 2 * BLK :], preferred_element_type=F32)
    keep = keep_ref[0]
    gate, up = gate_up[:, :BLK], gate_up[:, BLK:]
    sig = jax.nn.sigmoid(gate)
    act = keep * gate * sig
    dhid = keep * dhid
    hid[...] = (act * up).astype(BF16)
    dgu[:, BLK:] = (dhid * act).astype(BF16)
    dgu[:, :BLK] = (dhid * up * keep * sig * (1.0 + gate * (1.0 - sig))).astype(BF16)
    dims = (((0,), (0,)), ((), ()))
    for k, out in ((3, away1), (2, away0), (1, own1), (0, own0)):
        cols = slice(k * 512, (k + 1) * 512)
        gu = lax.dot_general(tok[:, cols], dgu[...], dims, preferred_element_type=F32)
        dn = lax.dot_general(cot[:, cols], hid[...], dims, preferred_element_type=F32)
        out[:, :, : 2 * BLK] = gu.astype(BF16).reshape(4, 128, 2 * BLK)
        out[:, :, 2 * BLK :] = dn.astype(BF16).reshape(4, 128, BLK)


def shard_kernel(gate, up, down, out):
    out[:, :BLK] = gate[...]
    out[:, BLK : 2 * BLK] = up[...]
    turned = down[...].T
    out[:64, 2 * BLK :] = turned[64:]
    out[64:, 2 * BLK :] = turned[:64]


def token_grads_kernel(place, dgu, w0, w1, w2, w3, r0, r1, r2, r3):
    side, core, parity, quarter = place[0], place[1], place[2], place[3]
    mask = halves_mask((TOK // 2, LANES), parity)
    dims = (((1,), (1,)), ((), ()))

    def half(weights, same, other):
        for k, w in enumerate(weights):
            wk = w[...].reshape(512, 3 * BLK)[:, : 2 * BLK]
            part = lax.dot_general(dgu[...], wk, dims, preferred_element_type=F32)
            for y in range(4):
                q = quarter ^ y
                at = (k ^ side) * 4 + (q & 1) * 2 + lax.shift_right_logical(q, 1)
                block = part[:, y * LANES : (y + 1) * LANES]
                top = block[: TOK // 2]
                low = pltpu.roll(block[TOK // 2 :], LANES // 2, 1)
                same[at] = jnp.where(mask, top, low).astype(BF16)
                other[at] = jnp.where(mask, low, top).astype(BF16)

    for turn, (first, second) in enumerate((((w0, w1), (w2, w3)), ((w2, w3), (w0, w1)))):

        @pl.when(core == turn)
        def _(first=first, second=second):
            half(first, r0, r1)
            half(second, r2, r3)


def call(kernel, outs, n_smem, n_in, scratch, mib):
    run = pl.pallas_call(
        kernel,
        out_shape=outs,
        in_specs=[SMEM] * n_smem + [VMEM] * n_in,
        out_specs=[VMEM] * len(outs),
        scratch_shapes=list(scratch),
        compiler_params=pltpu.CompilerParams(vmem_limit_bytes=mib * 1024 * 1024),
    )
    return run


def sds(*shape, dtype=BF16):
    return jax.ShapeDtypeStruct(shape, dtype)


def step(tokens, cotangent, gate_weight, up_weight, down_weight, width_steps, block_order):
    c, h = lax.axis_index("cand"), lax.axis_index("hid")
    parity = h % 2
    place = jnp.stack([(h // 4 ^ c // 2) % 2, (c ^ h // 2) % 2, parity, h // 8]).astype(jnp.int32)
    places = jnp.arange(block_order.shape[0], dtype=jnp.int32)
    logical = jnp.sum(jnp.where(places == h, block_order, 0))
    keep = (logical * BLK < width_steps[0] * (FF // 8)).astype(F32).reshape(1)

    t, u = tokens[0], cotangent[0]
    first, second = jnp.where(parity == 0, t, u), jnp.where(parity == 0, u, t)
    piece = jnp.concatenate([first, second], axis=1)[None]
    (shard,) = call(shard_kernel, [sds(128, 3 * BLK)], 0, 3, [], 4)(
        gate_weight, up_weight, down_weight
    )

    pieces = jnp.concatenate([piece, swap(piece, "hid", 16)], axis=0)
    far = swap(shard, "cand", 2)
    w_own = gather(shard, "cand", Y_GROUPS)
    pieces = jnp.concatenate([pieces, swap(pieces, "hid", 8)], axis=0)
    pieces, place, keep = lax.optimization_barrier((pieces, place, keep))
    others = swap(pieces, "hid", 4)
    los = [pieces] + [swap(pieces, "hid", b) for b in (1, 2, 3)]
    his = [others] + [swap(others, "hid", b) for b in (1, 2, 3)]
    w_far = gather(far, "cand", Y_GROUPS)
    weights = [w_own, w_far, swap(w_own, "cand", 1), swap(w_far, "cand", 1)]

    grad = sds(4, 128, 3 * BLK)
    own0, own1, away0, away1, dgu = call(
        forward_kernel, [grad] * 4 + [sds(TOK, 2 * BLK)], 2, 12,
        [pltpu.VMEM((TOK, 2048), BF16)] * 2 + [pltpu.VMEM((TOK, BLK), BF16)], 12,
    )(place, keep, *los, *his, *weights)
    r0, *rs = call(token_grads_kernel, [sds(8, 128, 128)] * 4, 1, 5, [], 8)(place, dgu, *weights)

    both1 = own1.astype(F32) + swap(away1, "cand", 1).astype(F32)
    total1 = total(exchange(both1.astype(BF16), "cand", Y_GROUPS))
    arrived0 = swap(away0, "cand", 1)
    both0 = (own0.astype(F32) + arrived0.astype(F32)).astype(BF16)
    grads = total(exchange(both0, "cand", Y_GROUPS))
    last = swap(total1.astype(BF16), "cand", 2)
    grads = lax.optimization_barrier(grads) + last.astype(F32)

    arrived = [swap(r, "hid", b) for b, r in zip((1, 2, 3), rs)]
    part = r0.astype(F32)
    for r in arrived:
        part = part + r.astype(F32)
    for dist in (1, 2, 4):
        n = part.shape[0] // 2
        r = swap(part[n:].astype(BF16), "hid", 4 * dist)
        part = part[:n] + r.astype(F32)
    part = part[0]
    left, right = part[:, :64], part[:, 64:]
    top, low = jnp.where(parity == 0, left, right), jnp.where(parity == 0, right, left)
    grad_tokens = jnp.concatenate([top, low], axis=0)[None]

    grad_down = grads[:, 2 * BLK :]
    grad_down = jnp.concatenate([grad_down[64:], grad_down[:64]], axis=0).T
    return grad_tokens, grads[:, :BLK], grads[:, BLK : 2 * BLK], grad_down


def solution(mesh):
    in_specs = (
        P("cand", None, "hid"),
        P("cand", None, "hid"),
        P("cand", "hid"),
        P("cand", "hid"),
        P("hid", "cand"),
        P("cand"),
        P(),
    )
    out_specs = (P("cand", None, "hid"), P("cand", "hid"), P("cand", "hid"), P("hid", "cand"))
    return jax.shard_map(step, mesh=mesh, in_specs=in_specs, out_specs=out_specs, check_vma=False)
```
